32 devices in a mesh: lat: 4 (over y, core), lon: 8 (over z, x).
Axes of the slice: x: 2, y: 2, z: 4, core: 2. Of those that a mesh axis runs over, the one named last changes fastest.
Arguments:
- field: float32 [64, 1024, 128], P('lon', 'lat'), may hold values from -6 to 6
- kappa: float32 [64, 1024], P('lon', 'lat'), may hold values from 0.06 to 0.24
- classes: int32 [64, 1024], P('lon', 'lat'), may hold values from 0 to 7
- inverses: float32 [8, 128, 128], replicated, as said below
Outputs:
- result: float32 [64, 1024, 128], P('lon', 'lat')
The draws below stay inside these ranges and needn't reach their ends.
Inputs may be any that keep to these rules, and one draw needn't show every extreme that they name: `inverses`: each matrix has diagonal entries between 0.4 and 1.0 and dense, full-rank off-diagonal entries of magnitude about 0.02; the matrices are not diagonally dominant.
All inputs are finite; a program needn't handle non-finite values.
Results may differ from the reference program's by a relative error of at most 0.00013.
Values sent between devices are 32-bit elements; how exact they have to be, the bound alone decides.
A program may use at most 64 MiB of HBM per device.

```python
import math
import jax
import jax.numpy as jnp
from jax import lax

LEV = 128
CLASSES = 8
STEPS = 6
NLON = 64
NLAT = 1024


def draw_inverses(key, part):
    key_diag = jax.random.fold_in(key, 11)
    key_off = jax.random.fold_in(key, 12)
    diag = jax.random.uniform(key_diag, (CLASSES, LEV), jnp.float32, 0.6, 1.0)
    off = 0.25 * jax.random.normal(key_off, (CLASSES, LEV, LEV), jnp.float32) / jnp.sqrt(jnp.float32(LEV))
    eye = jnp.eye(LEV, dtype=jnp.float32)
    return (off * (1.0 - eye) + diag[:, :, None] * eye).astype(jnp.float32)


def plant(entries, key, least, largest):
    place = [jax.random.randint(jax.random.fold_in(key, axis), (), 0, length) for axis, length in enumerate(entries.shape)]
    widest = entries.shape.index(max(entries.shape))
    beside = place[:widest] + [(place[widest] + 1) % entries.shape[widest]] + place[widest + 1:]
    return entries.at[tuple(place)].set(least).at[tuple(beside)].set(largest)


def block_levels(rng, dims, split, smallest, top_value):
    def one(position, blocks):
        heights = jax.random.uniform(jax.random.fold_in(jax.random.fold_in(rng, 6), position), (blocks,), jnp.float32, smallest / len(split), top_value / len(split))
        return jnp.repeat(jnp.exp(heights), dims[position] // blocks).reshape((-1,) + (1,) * (len(dims) - position - 1))

    loudness = one(*split[0])
    for cut in split[1:]:
        loudness = loudness * one(*cut)
    return loudness


def gaussian(own_key, extent, spread, reach, pieces=(), kind=jnp.bfloat16):
    array = jax.random.normal(own_key, extent, jnp.float32) * spread
    if len(pieces) > 0:
        array = block_levels(own_key, extent, pieces, -0.22, 0.18) * array
    return jnp.clip(array, min=-reach, max=reach).astype(kind)


def setup_inputs(seed: int = 0) -> dict:
    key_of = jax.random.split(jax.random.key(seed), 5)
    return {
        "field": gaussian(key_of[0], (NLON, NLAT, LEV), 1.0, 6.0, ((0, 8), (1, 4)), jnp.float32),
        "kappa": jnp.clip(jnp.exp(math.log(0.24) - 1.3862944 * jax.random.uniform(key_of[1], (NLON, NLAT), jnp.float32) ** block_levels(key_of[1], (NLON, NLAT), ((0, 8), (1, 4)), -0.2, 0.2)), 0.06, 0.24),
        "classes": plant(jax.random.randint(key_of[2], (NLON, NLAT), 0, CLASSES), jax.random.fold_in(key_of[2], 1), 0, CLASSES - 1).astype(jnp.int32),
        "inverses": draw_inverses(jax.random.fold_in(key_of[4], 71), 0),
    }


def explicit(field, kappa):
    east = jnp.roll(field, -1, 0)
    west = jnp.roll(field, 1, 0)
    k_east = jnp.roll(kappa, -1, 0)
    k_west = jnp.roll(kappa, 1, 0)
    padded = jnp.pad(field, ((0, 0), (1, 1), (0, 0)))
    k_padded = jnp.pad(kappa, ((0, 0), (1, 1)))
    north = padded[:, 2:]
    south = padded[:, :-2]
    k_north = k_padded[:, 2:]
    k_south = k_padded[:, :-2]
    total = (0.5 * (kappa + k_east))[..., None] * (east - field)
    total = total + (0.5 * (kappa + k_west))[..., None] * (west - field)
    total = total + (0.5 * (kappa + k_north))[..., None] * (north - field)
    total = total + (0.5 * (kappa + k_south))[..., None] * (south - field)
    return field + total


def vertical(field, classes, inverses):
    out = jnp.zeros(field.shape, jnp.float32)
    for kind in range(CLASSES):
        prod = jnp.einsum("xyl,ml->xym", field, inverses[kind], precision=lax.Precision.HIGHEST)
        out = out + jnp.where((classes == kind)[..., None], prod, jnp.float32(0.0))
    return out


def reference(field, kappa, classes, inverses):
    state = field
    for step in range(STEPS):
        state = vertical(explicit(state, kappa), classes, inverses)
    return state
```

```python
import functools

import jax
import jax.numpy as jnp
from jax import lax
from jax.experimental import pallas as pl
from jax.experimental.pallas import tpu as pltpu
from jax.sharding import PartitionSpec as P

STEPS = 6
EDGE = 8
PAD = 16
MESH = pl.DeviceIdType.MESH
F32 = jnp.float32
BF16 = jnp.bfloat16
AROUND = [(a, b) for a in (-1, 0, 1) for b in (-1, 0, 1) if (a, b) != (0, 0)]


def kernel(
    field, kappa, classes, inverses, out,
    u, neark, nearc, face_e, face_n, centre, parity, quad, weights,
    load_sem, send_k, recv_k, send_c, recv_c, send_e, recv_e, send_p, recv_p,
):
    nlon, nlat, lev = field.shape
    halo = STEPS
    span = nlon + 2 * halo
    low, high = PAD, PAD + nlat
    first, last = low - EDGE, high + EDGE
    rows = last - first
    lat, lon = lax.axis_index("lat"), lax.axis_index("lon")
    nlats, nlons = lax.axis_size("lat"), lax.axis_size("lon")
    has = {-1: lat > 0, 1: lat < nlats - 1}

    def device(dlat, dlon):
        return (lat + dlat, lax.rem(lon + dlon + nlons, nlons))

    loads = [
        pltpu.make_async_copy(
            field.at[j], u.at[0, halo + j, pl.ds(low, nlat)], load_sem.at[j]
        )
        for j in range(nlon)
    ]
    for load in loads:
        load.start()

    barrier = pltpu.get_barrier_semaphore()

    def guarded(dlat, action):
        if dlat == 0:
            action()
        else:
            pl.when(has[dlat])(action)

    for dlat in (-1, 0, 1):
        def greet(dlat=dlat):
            for a, b in AROUND:
                if a == dlat:
                    pl.semaphore_signal(
                        barrier, inc=1, device_id=device(a, b), device_id_type=MESH
                    )
        guarded(dlat, greet)
    peers = 2 + 3 * (has[-1].astype(jnp.int32) + has[1].astype(jnp.int32))
    pl.semaphore_wait(barrier, peers)

    small = []
    for n, (a, b) in enumerate(AROUND):
        for src, dst, ss, rs in (
            (kappa, neark, send_k, recv_k), (classes, nearc, send_c, recv_c)
        ):
            small.append((a, pltpu.make_async_remote_copy(
                src_ref=src, dst_ref=dst.at[1 - a, 1 - b],
                send_sem=ss.at[n], recv_sem=rs.at[n],
                device_id=device(a, b), device_id_type=MESH,
            )))
    lon_src = {-1: (halo, halo), 0: (halo, nlon), 1: (nlon, halo)}
    lon_dst = {-1: halo + nlon, 0: halo, 1: 0}
    edges = []
    for n, (a, b) in enumerate([ab for ab in AROUND if ab[0] != 0]):
        start, width = lon_src[b]
        edges.append((a, pltpu.make_async_remote_copy(
            src_ref=u.at[0, pl.ds(start, width), pl.ds(high - EDGE if a == 1 else low, EDGE)],
            dst_ref=u.at[0, pl.ds(lon_dst[b], width), pl.ds(first if a == 1 else high, EDGE)],
            send_sem=send_e.at[n], recv_sem=recv_e.at[n],
            device_id=device(a, b), device_id_type=MESH,
        )))
    planes = []
    for k in range(halo):
        for s, b in enumerate((1, -1)):
            src = halo + nlon - 1 - k if b == 1 else halo + k
            dst = halo - 1 - k if b == 1 else halo + nlon + k
            planes.append(pltpu.make_async_remote_copy(
                src_ref=u.at[0, src, pl.ds(low, nlat)],
                dst_ref=u.at[0, dst, pl.ds(low, nlat)],
                send_sem=send_p.at[2 * k + s], recv_sem=recv_p.at[2 * k + s],
                device_id=device(0, b), device_id_type=MESH,
            ))

    def start_all(group):
        for dlat in (0, -1, 1):
            def go(dlat=dlat):
                for a, copy in group:
                    if a == dlat:
                        copy.start()
            guarded(dlat, go)

    start_all(small)
    for load in loads:
        load.wait()
    start_all(edges)
    for copy in planes:
        copy.start()

    kinds = inverses.shape[0]
    for c in range(kinds):
        w = jnp.transpose(inverses[c])
        wh = w.astype(BF16)
        wl = (w - wh.astype(F32)).astype(BF16)
        r, q = (c % 2) * lev, (c // 2) * lev
        weights[pl.ds(r, lev), pl.ds(q, lev)] = wh
        weights[pl.ds(2 * lev + r, lev), pl.ds(q, lev)] = wh
        weights[pl.ds(4 * lev + r, lev), pl.ds(q, lev)] = wl

    for a in (-1, 1):
        @pl.when(jnp.logical_not(has[a]))
        def _(a=a):
            for b in range(3):
                neark[1 + a, b] = jnp.zeros((nlon, nlat), F32)
                nearc[1 + a, b] = jnp.zeros((nlon, nlat), jnp.int32)
            edge = first if a == -1 else high
            u[0, :, pl.ds(edge, EDGE)] = jnp.zeros((span, EDGE, lev), F32)

    def wait_all(group):
        for dlat in (0, -1, 1):
            def go(dlat=dlat):
                for a, copy in group:
                    if -a == dlat:
                        copy.wait_recv()
            guarded(dlat, go)

    wait_all(small)
    neark[1, 1] = kappa[...]
    nearc[1, 1] = classes[...]

    def turned(near):
        strips = []
        for b in range(3):
            strips.append(jnp.concatenate(
                [near[0, b][:, nlat - 128:], near[1, b], near[2, b][:, :128]], axis=1
            ).astype(F32))
        lines = jnp.concatenate(
            strips + [jnp.zeros((128 - 3 * nlon, nlat + 256), F32)], axis=0
        )
        tall = jnp.concatenate(
            [jnp.transpose(lines[:, g:g + 128]) for g in range(0, nlat + 256, 128)], axis=0
        )
        return tall[128 - PAD:128 + nlat + PAD]

    kt = turned(neark)
    ct = turned(nearc)
    total = nlat + 2 * PAD
    at = lat * nlat - PAD + lax.broadcasted_iota(jnp.int32, (total, 128), 0)
    inside = jnp.where((at >= 0) & (at < nlat * nlats), 1.0, 0.0).astype(F32)
    ke = 0.5 * (kt + pltpu.roll(kt, 127, 1))
    kw = pltpu.roll(ke, 1, 1)
    kn = 0.5 * (kt + pltpu.roll(kt, total - 1, 0))
    ks = pltpu.roll(kn, 1, 0)
    c0 = (1.0 - (ke + kw + kn + ks)) * inside
    fe = ke * inside
    fn = kn * inside * pltpu.roll(inside, total - 1, 0)
    half = jnp.floor(ct * 0.5)
    odd = ct - 2.0 * half
    shift = nlon - halo
    for p in range(span):
        def wide(x):
            return jnp.broadcast_to(x[:, p + shift:p + shift + 1], (total, lev))
        face_e[p] = wide(fe)
        face_n[p] = wide(fn)
        centre[p] = wide(c0)
        quad[p] = wide(half)
        parity[p] = wide(odd)[first:last].astype(BF16)

    wait_all(edges)

    mid = pl.ds(first, rows)
    up = pl.ds(first + 1, rows)
    down = pl.ds(first - 1, rows)

    def pair(t, i):
        sides = (i, span - 1 - i)
        lhs = []
        for p in sides:
            v = centre[p, mid] * u[t - 1, p, mid]
            v = v + face_e[p, mid] * u[t - 1, p + 1, mid]
            v = v + face_e[p - 1, mid] * u[t - 1, p - 1, mid]
            v = v + face_n[p, mid] * u[t - 1, p, up]
            v = v + face_n[p, down] * u[t - 1, p, down]
            vh = v.astype(BF16)
            vl = (v - vh.astype(F32)).astype(BF16)
            odds = parity[p]
            ho = vh * odds
            he = vh - ho
            lo = vl * odds
            le = vl - lo
            lhs.append(jnp.concatenate([he, ho, le, lo, he, ho], axis=1))
        res = jnp.dot(
            jnp.concatenate(lhs, axis=0), weights[...], preferred_element_type=F32
        )
        for n, p in enumerate(sides):
            r = res[n * rows:(n + 1) * rows]
            kind = quad[p, mid]
            pick = r[:, :lev]
            for q in range(1, kinds // 2):
                pick = jnp.where(kind == float(q), r[:, q * lev:(q + 1) * lev], pick)
            u[t, p, mid] = pick

    def finish(i):
        for p in (i, span - 1 - i):
            out[p - halo] = u[STEPS, p, pl.ds(low, nlat)]

    for t in range(1, STEPS + 1):
        def inner(i, carry, t=t):
            pair(t, i)
            return carry
        if halo + t < span // 2:
            lax.fori_loop(halo + t, span // 2, inner, 0)
    for k in range(1, halo + 1):
        planes[2 * k - 2].wait_recv()
        planes[2 * k - 1].wait_recv()
        top = min(STEPS, span // 2 - 1 - halo + k)

        def wave(t, carry, k=k):
            pair(t, halo - k + t)
            return carry
        lax.fori_loop(1, top + 1, wave, 0)
        if top == STEPS:
            finish(halo - k + STEPS)

    for group in (small, edges):
        for dlat in (0, -1, 1):
            def done(dlat=dlat, group=group):
                for a, copy in group:
                    if a == dlat:
                        copy.wait_send()
            guarded(dlat, done)
    for copy in planes:
        copy.wait_send()


def body(field, kappa, classes, inverses):
    nlon, nlat, lev = field.shape
    span = nlon + 2 * STEPS
    total = nlat + 2 * PAD
    kinds = inverses.shape[0]
    vmem = pl.BlockSpec(memory_space=pltpu.VMEM)
    dma = pltpu.SemaphoreType.DMA
    return pl.pallas_call(
        kernel,
        out_shape=jax.ShapeDtypeStruct(field.shape, F32),
        in_specs=[pl.BlockSpec(memory_space=pl.ANY), vmem, vmem, vmem],
        out_specs=vmem,
        scratch_shapes=[
            pltpu.VMEM((STEPS + 1, span, total, lev), F32),
            pltpu.VMEM((3, 3, nlon, nlat), F32),
            pltpu.VMEM((3, 3, nlon, nlat), jnp.int32),
            pltpu.VMEM((span, total, lev), F32),
            pltpu.VMEM((span, total, lev), F32),
            pltpu.VMEM((span, total, lev), F32),
            pltpu.VMEM((span, total - 2 * (PAD - EDGE), lev), BF16),
            pltpu.VMEM((span, total, lev), F32),
            pltpu.VMEM((6 * lev, kinds // 2 * lev), BF16),
            dma((nlon,)), dma((8,)), dma((8,)), dma((8,)), dma((8,)),
            dma((6,)), dma((6,)), dma((2 * STEPS,)), dma((2 * STEPS,)),
        ],
        compiler_params=pltpu.CompilerParams(
            collective_id=0, has_side_effects=True, vmem_limit_bytes=60 * 1024 * 1024
        ),
    )(field, kappa, classes, inverses)


def solution(mesh):
    return jax.shard_map(
        body,
        mesh=mesh,
        in_specs=(P("lon", "lat", None), P("lon", "lat"), P("lon", "lat"), P()),
        out_specs=P("lon", "lat", None),
        check_vma=False,
    )
```

```python
import functools

import jax
import jax.numpy as jnp
from jax import lax
from jax.experimental import pallas as pl
from jax.experimental.pallas import tpu as pltpu
from jax.sharding import PartitionSpec as P

STEPS = 6
EDGE = 8
PAD = 16
MESH = pl.DeviceIdType.MESH
F32 = jnp.float32
BF16 = jnp.bfloat16


def kernel(
    field, kappa, classes, inverses, out,
    u, mine, final, neark, nearc, face_e, face_n, centre, parity, quad, weights,
    load_sem, own_sem, store_sem, send_k, recv_k, send_c, recv_c,
    send_e, recv_e, send_p, recv_p,
):
    nlon, nlat, lev = field.shape
    halo = STEPS
    span = 2 * (nlon + halo)
    half = nlat // 2
    total = half + 2 * PAD
    low, high = PAD, PAD + half
    first, last = low - EDGE, high + EDGE
    rows = last - first
    main = half + EDGE
    lat, lon = lax.axis_index("lat"), lax.axis_index("lon")
    nlats, nlons = lax.axis_size("lat"), lax.axis_size("lon")
    s = lax.rem(lon, 2)
    g = 1 - 2 * s
    d = -g
    has_out = jnp.logical_and(lat + d >= 0, lat + d < nlats)
    has_in = jnp.logical_and(lat - d >= 0, lat - d < nlats)

    def device(dlat, dlon):
        return (lat + dlat, lax.rem(lon + dlon + nlons, nlons))

    def place(n):
        return (nlon - 1) * s + g * n

    def main_src(q):
        return pl.multiple_of((half - EDGE) * q, EDGE)

    def main_dst(q):
        return pl.multiple_of(low - EDGE * q, EDGE)

    def outer_src(q):
        return pl.multiple_of((nlat - EDGE) * (1 - q), EDGE)

    def outer_dst(q):
        return pl.multiple_of(first + main * q, EDGE)

    order = list(range(nlon))[::-1]
    loads = {}
    for n in order:
        loads[n] = pltpu.make_async_copy(field.at[place(n)], mine.at[n], load_sem.at[n])
        loads[n].start()
    owns = [
        pltpu.make_async_copy(
            field.at[place(n), pl.ds(main_src(s), main)],
            u.at[0, halo + n, pl.ds(main_dst(s), main)],
            own_sem.at[n],
        )
        for n in range(nlon)
    ]
    for copy in owns:
        copy.start()

    barrier = pltpu.get_barrier_semaphore()

    def greet(dlat, dlons):
        for dlon in dlons:
            pl.semaphore_signal(
                barrier, inc=1, device_id=device(dlat, dlon), device_id_type=MESH
            )

    greet(0, (g, -g, 2 * g, -2 * g))

    @pl.when(has_in)
    def _():
        greet(-d, (0, -2 * g))

    @pl.when(has_out)
    def _():
        greet(d, (0, g, -g, 2 * g))

    pl.semaphore_wait(
        barrier, 4 + 2 * has_in.astype(jnp.int32) + 4 * has_out.astype(jnp.int32)
    )

    targets = [
        (0, g, 0, 2), (0, -g, 0, 0), (0, -2 * g, 0, 3),
        (-d, 0, 1, 1), (-d, -2 * g, 1, 3),
        (d, g, 1, 2), (d, -g, 1, 0),
    ]
    small = []
    for n, (a, b, outer, slot) in enumerate(targets):
        for src, dst, ss, rs in (
            (kappa, neark, send_k, recv_k), (classes, nearc, send_c, recv_c)
        ):
            small.append(pltpu.make_async_remote_copy(
                src_ref=src, dst_ref=dst.at[outer, slot],
                send_sem=ss.at[n], recv_sem=rs.at[n],
                device_id=device(a, b), device_id_type=MESH,
            ))
    small_near, small_in, small_out = small[:6], small[6:10], small[10:]

    edge_count = [0]

    def edge(src, dst, q, a, b):
        n = edge_count[0]
        edge_count[0] += 1
        return pltpu.make_async_remote_copy(
            src_ref=src.at[:, pl.ds(outer_src(q), EDGE)],
            dst_ref=dst.at[:, pl.ds(outer_dst(q), EDGE)],
            send_sem=send_e.at[n], recv_sem=recv_e.at[n],
            device_id=device(a, b), device_id_type=MESH,
        )

    begin = u.at[0]
    edges_in = [
        edge(mine, begin.at[pl.ds(halo, nlon)], s, -d, 0),
        edge(mine.at[pl.ds(0, halo)], begin.at[pl.ds(halo + 2 * nlon, halo)], s, -d, -2 * g),
    ]
    edges_out = [
        edge(mine.at[pl.ds(n, 1)], begin.at[pl.ds(span - 1 - halo - n, 1)], 1 - s, d, g)
        for n in range(nlon)
    ] + [
        edge(mine.at[pl.ds(n, 1)], begin.at[pl.ds(halo - 1 - n, 1)], 1 - s, d, -g)
        for n in range(halo)
    ]

    def plane(n, src, dst, b):
        return pltpu.make_async_remote_copy(
            src_ref=src, dst_ref=dst, send_sem=send_p.at[n], recv_sem=recv_p.at[n],
            device_id=device(0, b), device_id_type=MESH,
        )

    swaps = [
        plane(
            n,
            mine.at[nlon - 1 - n, pl.ds(main_src(1 - s), main)],
            u.at[0, halo + nlon + n, pl.ds(main_dst(1 - s), main)],
            g,
        )
        for n in range(nlon)
    ]
    direct = [
        plane(
            nlon + n,
            mine.at[n, pl.ds(main_src(s), main)],
            u.at[0, halo + 2 * nlon + n, pl.ds(main_dst(s), main)],
            -2 * g,
        )
        for n in range(halo)
    ]
    relays = [
        plane(
            nlon + halo + n,
            u.at[0, 2 * nlon + n, pl.ds(main_dst(s), main)],
            u.at[0, n, pl.ds(main_dst(s), main)],
            2 * g,
        )
        for n in range(halo)
    ]
    returns = [
        plane(
            nlon + 2 * halo + n,
            u.at[STEPS, halo + nlon + n, pl.ds(low, half)],
            final.at[nlon - 1 - n],
            g,
        )
        for n in range(nlon)
    ]

    for copy in small_near:
        copy.start()

    @pl.when(has_in)
    def _():
        for copy in small_in:
            copy.start()

    @pl.when(has_out)
    def _():
        for copy in small_out:
            copy.start()

    for n in order:
        loads[n].wait()
        swaps[nlon - 1 - n].start()
    for copy in direct:
        copy.start()

    @pl.when(has_in)
    def _():
        for copy in edges_in:
            copy.start()

    @pl.when(has_out)
    def _():
        for copy in edges_out:
            copy.start()

    kinds = inverses.shape[0]
    for c in range(kinds):
        w = jnp.transpose(inverses[c])
        wh = w.astype(BF16)
        wl = (w - wh.astype(F32)).astype(BF16)
        r, q = (c % 2) * lev, (c // 2) * lev
        weights[pl.ds(r, lev), pl.ds(q, lev)] = wh
        weights[pl.ds(2 * lev + r, lev), pl.ds(q, lev)] = wh
        weights[pl.ds(4 * lev + r, lev), pl.ds(q, lev)] = wl

    @pl.when(jnp.logical_not(has_out))
    def _():
        for slot in range(4):
            neark[1, slot] = jnp.zeros((nlon, nlat), F32)
            nearc[1, slot] = jnp.zeros((nlon, nlat), jnp.int32)
        u[0, :, pl.ds(outer_dst(s), EDGE)] = jnp.zeros((span, EDGE, lev), F32)

    neark[0, 1] = kappa[...]
    nearc[0, 1] = classes[...]
    for copy in small_near:
        copy.wait_recv()

    @pl.when(has_out)
    def _():
        for copy in small_in + small_out:
            copy.wait_recv()

    upright = s == 0

    def turned(near):
        strips = []
        for slot in range(4):
            here, there = near[0, slot].astype(F32), near[1, slot].astype(F32)
            line = jnp.where(
                upright,
                jnp.concatenate([there[:, nlat - 128:], here[:, :half + 128]], axis=1),
                jnp.concatenate([here[:, half - 128:], there[:, :128]], axis=1),
            )
            back = jnp.concatenate([line[n:n + 1] for n in range(nlon)[::-1]], axis=0)
            strips.append(jnp.where(upright, line, back))
        lines = jnp.concatenate(
            strips + [jnp.zeros((128 - 4 * nlon, half + 256), F32)], axis=0
        )
        tall = jnp.concatenate(
            [jnp.transpose(lines[:, c:c + 128]) for c in range(0, half + 256, 128)], axis=0
        )
        return tall[128 - PAD:128 + half + PAD]

    kt = turned(neark)
    ct = turned(nearc)
    at = lat * nlat + half * s - PAD + lax.broadcasted_iota(jnp.int32, (total, 128), 0)
    inside = jnp.where((at >= 0) & (at < nlat * nlats), 1.0, 0.0).astype(F32)
    ke = 0.5 * (kt + pltpu.roll(kt, 127, 1))
    kw = pltpu.roll(ke, 1, 1)
    kn = 0.5 * (kt + pltpu.roll(kt, total - 1, 0))
    ks = pltpu.roll(kn, 1, 0)
    c0 = (1.0 - (ke + kw + kn + ks)) * inside
    fe = ke * inside
    fn = kn * inside * pltpu.roll(inside, total - 1, 0)
    whole = jnp.floor(ct * 0.5)
    odd = ct - 2.0 * whole
    shift = nlon - halo
    for p in range(span):
        def wide(x):
            return jnp.broadcast_to(x[:, p + shift:p + shift + 1], (total, lev))
        face_e[p] = wide(fe)
        face_n[p] = wide(fn)
        centre[p] = wide(c0)
        quad[p] = wide(whole)
        parity[p] = wide(odd)[first:last].astype(BF16)

    for copy in owns:
        copy.wait()

    @pl.when(has_out)
    def _():
        for copy in edges_in + edges_out:
            copy.wait_recv()

    mid = pl.ds(first, rows)
    up = pl.ds(first + 1, rows)
    down = pl.ds(first - 1, rows)

    def pair(t, i):
        sides = (i, i + 1)
        lhs = []
        for p in sides:
            v = centre[p, mid] * u[t - 1, p, mid]
            v = v + face_e[p, mid] * u[t - 1, p + 1, mid]
            v = v + face_e[p - 1, mid] * u[t - 1, p - 1, mid]
            v = v + face_n[p, mid] * u[t - 1, p, up]
            v = v + face_n[p, down] * u[t - 1, p, down]
            vh = v.astype(BF16)
            vl = (v - vh.astype(F32)).astype(BF16)
            odds = parity[p]
            ho = vh * odds
            he = vh - ho
            lo = vl * odds
            le = vl - lo
            lhs.append(jnp.concatenate([he, ho, le, lo, he, ho], axis=1))
        res = jnp.dot(
            jnp.concatenate(lhs, axis=0), weights[...], preferred_element_type=F32
        )
        for n, p in enumerate(sides):
            r = res[n * rows:(n + 1) * rows]
            kind = quad[p, mid]
            pick = r[:, :lev]
            for q in range(1, kinds // 2):
                pick = jnp.where(kind == float(q), r[:, q * lev:(q + 1) * lev], pick)
            u[t, p, mid] = pick

    def store(n):
        return pltpu.make_async_copy(
            u.at[STEPS, halo + n, pl.ds(low, half)],
            out.at[place(n), pl.ds(pl.multiple_of(half * s, EDGE), half)],
            store_sem.at[n],
        )

    for t in range(1, STEPS + 1):
        def inner(i, carry, t=t):
            pair(t, halo + t + 2 * i)
            return carry
        count = nlon // 2 - t
        if count > 0:
            lax.fori_loop(0, count, inner, 0)

    def done(p):
        if halo <= p < halo + nlon:
            store(p - halo).start()
        elif halo + nlon <= p < halo + 2 * nlon:
            returns[p - halo - nlon].start()

    for b in range(halo + nlon, span, 2):
        for p in (b, b + 1):
            if p < halo + 2 * nlon:
                swaps[p - halo - nlon].wait_recv()
                if p >= 2 * nlon:
                    relays[p - 2 * nlon].start()
            else:
                direct[p - halo - 2 * nlon].wait_recv()
        top = min(STEPS, (b - halo) // 2)

        def wave(t, carry, b=b):
            pair(t, b - t)
            return carry
        lax.fori_loop(1, top + 1, wave, 0)
        if top == STEPS:
            done(b - STEPS)
            done(b + 1 - STEPS)
    for a in range(halo - 2, -1, -2):
        relays[a + 1].wait_recv()
        relays[a].wait_recv()

        def wave_left(t, carry, a=a):
            pair(t, a + t)
            return carry
        lax.fori_loop(1, STEPS + 1, wave_left, 0)
        done(a + STEPS)
        done(a + 1 + STEPS)

    def store_back(n):
        return pltpu.make_async_copy(
            final.at[n],
            out.at[place(n), pl.ds(pl.multiple_of(half * (1 - s), EDGE), half)],
            store_sem.at[nlon + n],
        )

    for n in range(nlon):
        returns[n].wait_recv()
        store_back(nlon - 1 - n).start()

    for copy in small_near + swaps + direct + relays + returns:
        copy.wait_send()

    @pl.when(has_in)
    def _():
        for copy in small_in + edges_in:
            copy.wait_send()

    @pl.when(has_out)
    def _():
        for copy in small_out + edges_out:
            copy.wait_send()

    for n in range(nlon):
        store(n).wait()
        store_back(n).wait()


def body(field, kappa, classes, inverses):
    nlon, nlat, lev = field.shape
    span = 2 * (nlon + STEPS)
    half = nlat // 2
    total = half + 2 * PAD
    kinds = inverses.shape[0]
    vmem = pl.BlockSpec(memory_space=pltpu.VMEM)
    anywhere = pl.BlockSpec(memory_space=pl.ANY)
    dma = pltpu.SemaphoreType.DMA
    planes = 2 * nlon + 2 * STEPS
    edges = 2 + nlon + STEPS
    return pl.pallas_call(
        kernel,
        out_shape=jax.ShapeDtypeStruct(field.shape, F32),
        in_specs=[anywhere, vmem, vmem, vmem],
        out_specs=anywhere,
        scratch_shapes=[
            pltpu.VMEM((STEPS + 1, span, total, lev), F32),
            pltpu.VMEM((nlon, nlat, lev), F32),
            pltpu.VMEM((nlon, half, lev), F32),
            pltpu.VMEM((2, 4, nlon, nlat), F32),
            pltpu.VMEM((2, 4, nlon, nlat), jnp.int32),
            pltpu.VMEM((span, total, lev), F32),
            pltpu.VMEM((span, total, lev), F32),
            pltpu.VMEM((span, total, lev), F32),
            pltpu.VMEM((span, total - 2 * (PAD - EDGE), lev), BF16),
            pltpu.VMEM((span, total, lev), F32),
            pltpu.VMEM((6 * lev, kinds // 2 * lev), BF16),
            dma((nlon,)), dma((nlon,)), dma((2 * nlon,)),
            dma((7,)), dma((7,)), dma((7,)), dma((7,)),
            dma((edges,)), dma((edges,)), dma((planes,)), dma((planes,)),
        ],
        compiler_params=pltpu.CompilerParams(
            collective_id=0, has_side_effects=True, vmem_limit_bytes=60 * 1024 * 1024
        ),
    )(field, kappa, classes, inverses)


def solution(mesh):
    return jax.shard_map(
        body,
        mesh=mesh,
        in_specs=(P("lon", "lat", None), P("lon", "lat"), P("lon", "lat"), P()),
        out_specs=P("lon", "lat", None),
        check_vma=False,
    )
```

```python
import functools

import jax
import jax.numpy as jnp
from jax import lax
from jax.experimental import pallas as pl
from jax.experimental.pallas import tpu as pltpu
from jax.sharding import PartitionSpec as P

STEPS = 6
EDGE = 8
PAD = 16
MESH = pl.DeviceIdType.MESH
F32 = jnp.float32
BF16 = jnp.bfloat16


def kernel(
    field, kappa, classes, inverses, out,
    u, mine, final, neark, nearc, face_e, face_n, centre, parity, quad, weights,
    load_sem, own_sem, store_sem, send_k, recv_k, send_c, recv_c,
    send_e, recv_e, send_p, recv_p,
):
    nlon, nlat, lev = field.shape
    halo = STEPS
    span = 2 * (nlon + halo)
    half = nlat // 2
    total = half + 2 * PAD
    low, high = PAD, PAD + half
    first, last = low - EDGE, high + EDGE
    rows = last - first
    main = half + EDGE
    lat, lon = lax.axis_index("lat"), lax.axis_index("lon")
    nlats, nlons = lax.axis_size("lat"), lax.axis_size("lon")
    s = lax.rem(lon, 2)
    g = 1 - 2 * s
    d = -g
    has_out = jnp.logical_and(lat + d >= 0, lat + d < nlats)
    has_in = jnp.logical_and(lat - d >= 0, lat - d < nlats)

    def device(dlat, dlon):
        return (lat + dlat, lax.rem(lon + dlon + nlons, nlons))

    def place(n):
        return (nlon - 1) * s + g * n

    def main_src(q):
        return pl.multiple_of((half - EDGE) * q, EDGE)

    def main_dst(q):
        return pl.multiple_of(low - EDGE * q, EDGE)

    def outer_src(q):
        return pl.multiple_of((nlat - EDGE) * (1 - q), EDGE)

    def outer_dst(q):
        return pl.multiple_of(first + main * q, EDGE)

    order = list(range(nlon))[::-1]
    loads = {}
    for n in order:
        loads[n] = pltpu.make_async_copy(field.at[place(n)], mine.at[n], load_sem.at[n])
        loads[n].start()
    owns = [
        pltpu.make_async_copy(
            field.at[place(n), pl.ds(main_src(s), main)],
            u.at[0, halo + n, pl.ds(main_dst(s), main)],
            own_sem.at[n],
        )
        for n in range(nlon)
    ]
    for copy in owns:
        copy.start()

    barrier = pltpu.get_barrier_semaphore()

    def greet(dlat, dlons):
        for dlon in dlons:
            pl.semaphore_signal(
                barrier, inc=1, device_id=device(dlat, dlon), device_id_type=MESH
            )

    greet(0, (g, -g, 2 * g, -2 * g))

    @pl.when(has_in)
    def _():
        greet(-d, (0, -2 * g))

    @pl.when(has_out)
    def _():
        greet(d, (0, g, -g, 2 * g))

    pl.semaphore_wait(
        barrier, 4 + 2 * has_in.astype(jnp.int32) + 4 * has_out.astype(jnp.int32)
    )

    targets = [
        (0, g, 0, 2), (0, -g, 0, 0), (0, -2 * g, 0, 3),
        (-d, 0, 1, 1), (-d, -2 * g, 1, 3),
        (d, g, 1, 2), (d, -g, 1, 0),
    ]
    small = []
    for n, (a, b, outer, slot) in enumerate(targets):
        for src, dst, ss, rs in (
            (kappa, neark, send_k, recv_k), (classes, nearc, send_c, recv_c)
        ):
            small.append(pltpu.make_async_remote_copy(
                src_ref=src, dst_ref=dst.at[outer, slot],
                send_sem=ss.at[n], recv_sem=rs.at[n],
                device_id=device(a, b), device_id_type=MESH,
            ))
    small_near, small_in, small_out = small[:6], small[6:10], small[10:]

    edge_count = [0]

    def edge(src, dst, q, a, b):
        n = edge_count[0]
        edge_count[0] += 1
        return pltpu.make_async_remote_copy(
            src_ref=src.at[:, pl.ds(outer_src(q), EDGE)],
            dst_ref=dst.at[:, pl.ds(outer_dst(q), EDGE)],
            send_sem=send_e.at[n], recv_sem=recv_e.at[n],
            device_id=device(a, b), device_id_type=MESH,
        )

    begin = u.at[0]
    edges_in = [
        edge(mine, begin.at[pl.ds(halo, nlon)], s, -d, 0),
        edge(mine.at[pl.ds(0, halo)], begin.at[pl.ds(halo + 2 * nlon, halo)], s, -d, -2 * g),
    ]
    edges_out = [
        edge(mine.at[pl.ds(n, 1)], begin.at[pl.ds(span - 1 - halo - n, 1)], 1 - s, d, g)
        for n in range(nlon)
    ] + [
        edge(mine.at[pl.ds(n, 1)], begin.at[pl.ds(halo - 1 - n, 1)], 1 - s, d, -g)
        for n in range(halo)
    ]

    def plane(n, src, dst, b):
        return pltpu.make_async_remote_copy(
            src_ref=src, dst_ref=dst, send_sem=send_p.at[n], recv_sem=recv_p.at[n],
            device_id=device(0, b), device_id_type=MESH,
        )

    swaps = [
        plane(
            n,
            mine.at[nlon - 1 - n, pl.ds(main_src(1 - s), main)],
            u.at[0, halo + nlon + n, pl.ds(main_dst(1 - s), main)],
            g,
        )
        for n in range(nlon)
    ]
    direct = [
        plane(
            nlon + n,
            mine.at[n, pl.ds(main_src(s), main)],
            u.at[0, halo + 2 * nlon + n, pl.ds(main_dst(s), main)],
            -2 * g,
        )
        for n in range(halo)
    ]
    relays = [
        plane(
            nlon + halo + n,
            u.at[0, 2 * nlon + n, pl.ds(main_dst(s), main)],
            u.at[0, n, pl.ds(main_dst(s), main)],
            2 * g,
        )
        for n in range(halo)
    ]
    returns = [
        plane(
            nlon + 2 * halo + n,
            u.at[STEPS, halo + nlon + n, pl.ds(low, half)],
            final.at[nlon - 1 - n],
            g,
        )
        for n in range(nlon)
    ]

    for copy in small_near:
        copy.start()

    @pl.when(has_in)
    def _():
        for copy in small_in:
            copy.start()

    @pl.when(has_out)
    def _():
        for copy in small_out:
            copy.start()

    for n in order:
        loads[n].wait()

    @pl.when(has_in)
    def _():
        for copy in edges_in:
            copy.start()

    @pl.when(has_out)
    def _():
        for copy in edges_out:
            copy.start()

    for copy in swaps + direct:
        copy.start()

    kinds = inverses.shape[0]
    for c in range(kinds):
        w = jnp.transpose(inverses[c])
        wh = w.astype(BF16)
        wl = (w - wh.astype(F32)).astype(BF16)
        r, q = (c % 2) * lev, (c // 2) * lev
        weights[pl.ds(r, lev), pl.ds(q, lev)] = wh
        weights[pl.ds(2 * lev + r, lev), pl.ds(q, lev)] = wh
        weights[pl.ds(4 * lev + r, lev), pl.ds(q, lev)] = wl

    @pl.when(jnp.logical_not(has_out))
    def _():
        for slot in range(4):
            neark[1, slot] = jnp.zeros((nlon, nlat), F32)
            nearc[1, slot] = jnp.zeros((nlon, nlat), jnp.int32)
        u[0, :, pl.ds(outer_dst(s), EDGE)] = jnp.zeros((span, EDGE, lev), F32)

    neark[0, 1] = kappa[...]
    nearc[0, 1] = classes[...]
    for copy in small_near:
        copy.wait_recv()

    @pl.when(has_out)
    def _():
        for copy in small_in + small_out:
            copy.wait_recv()

    upright = s == 0

    def turned(near):
        strips = []
        for slot in range(4):
            here, there = near[0, slot].astype(F32), near[1, slot].astype(F32)
            line = jnp.where(
                upright,
                jnp.concatenate([there[:, nlat - 128:], here[:, :half + 128]], axis=1),
                jnp.concatenate([here[:, half - 128:], there[:, :128]], axis=1),
            )
            back = jnp.concatenate([line[n:n + 1] for n in range(nlon)[::-1]], axis=0)
            strips.append(jnp.where(upright, line, back))
        lines = jnp.concatenate(
            strips + [jnp.zeros((128 - 4 * nlon, half + 256), F32)], axis=0
        )
        tall = jnp.concatenate(
            [jnp.transpose(lines[:, c:c + 128]) for c in range(0, half + 256, 128)], axis=0
        )
        return tall[128 - PAD:128 + half + PAD]

    kt = turned(neark)
    ct = turned(nearc)
    at = lat * nlat + half * s - PAD + lax.broadcasted_iota(jnp.int32, (total, 128), 0)
    inside = jnp.where((at >= 0) & (at < nlat * nlats), 1.0, 0.0).astype(F32)
    ke = 0.5 * (kt + pltpu.roll(kt, 127, 1))
    kw = pltpu.roll(ke, 1, 1)
    kn = 0.5 * (kt + pltpu.roll(kt, total - 1, 0))
    ks = pltpu.roll(kn, 1, 0)
    c0 = (1.0 - (ke + kw + kn + ks)) * inside
    fe = ke * inside
    fn = kn * inside * pltpu.roll(inside, total - 1, 0)
    whole = jnp.floor(ct * 0.5)
    odd = ct - 2.0 * whole
    shift = nlon - halo
    for p in range(span):
        def wide(x):
            return jnp.broadcast_to(x[:, p + shift:p + shift + 1], (total, lev))
        face_e[p] = wide(fe)
        face_n[p] = wide(fn)
        centre[p] = wide(c0)
        quad[p] = wide(whole)
        parity[p] = wide(odd)[first:last].astype(BF16)

    for copy in owns:
        copy.wait()

    @pl.when(has_out)
    def _():
        edges_in[0].wait_recv()

    mid = pl.ds(first, rows)
    up = pl.ds(first + 1, rows)
    down = pl.ds(first - 1, rows)

    def columns(t, sides):
        lhs = []
        for p in sides:
            v = centre[p, mid] * u[t - 1, p, mid]
            v = v + face_e[p, mid] * u[t - 1, p + 1, mid]
            v = v + face_e[p - 1, mid] * u[t - 1, p - 1, mid]
            v = v + face_n[p, mid] * u[t - 1, p, up]
            v = v + face_n[p, down] * u[t - 1, p, down]
            vh = v.astype(BF16)
            vl = (v - vh.astype(F32)).astype(BF16)
            odds = parity[p]
            ho = vh * odds
            he = vh - ho
            lo = vl * odds
            le = vl - lo
            lhs.append(jnp.concatenate([he, ho, le, lo, he, ho], axis=1))
        res = jnp.dot(
            jnp.concatenate(lhs, axis=0), weights[...], preferred_element_type=F32
        )
        for n, p in enumerate(sides):
            r = res[n * rows:(n + 1) * rows]
            kind = quad[p, mid]
            pick = r[:, :lev]
            for q in range(1, kinds // 2):
                pick = jnp.where(kind == float(q), r[:, q * lev:(q + 1) * lev], pick)
            u[t, p, mid] = pick

    def store(n):
        return pltpu.make_async_copy(
            u.at[STEPS, halo + n, pl.ds(low, half)],
            out.at[place(n), pl.ds(pl.multiple_of(half * s, EDGE), half)],
            store_sem.at[n],
        )

    for t in range(1, STEPS + 1):
        def inner(i, carry, t=t):
            columns(t, (halo + t + 2 * i, halo + t + 2 * i + 1))
            return carry
        count = nlon // 2 - t
        if count > 0:
            lax.fori_loop(0, count, inner, 0)

    @pl.when(has_out)
    def _():
        for copy in edges_in[1:] + edges_out:
            copy.wait_recv()

    def done(p):
        if halo <= p < halo + nlon:
            store(p - halo).start()
        elif halo + nlon <= p < halo + 2 * nlon:
            returns[p - halo - nlon].start()

    def arrive(p):
        if p < halo:
            relays[p].wait_recv()
        elif p < halo + 2 * nlon:
            swaps[p - halo - nlon].wait_recv()
            if p >= 2 * nlon:
                relays[p - 2 * nlon].start()
        else:
            direct[p - halo - 2 * nlon].wait_recv()

    right = list(range(halo + nlon, span))
    left = list(range(halo))[::-1]
    cut = STEPS - nlon // 2
    waves = [(right[2 * n:2 * n + 2], []) for n in range(cut)]
    rest = right[2 * cut:]
    while len(rest) >= 4:
        waves.append((rest[:4], []))
        rest = rest[4:]
    waves.append((rest, left[:4 - len(rest)]))
    left = left[4 - len(rest):]
    while left:
        waves.append(([], left[:4]))
        left = left[4:]
    for east, west in waves:
        for p in east + west:
            arrive(p)
        top = min([STEPS] + [(p - halo) // 2 for p in east])

        def wave(t, carry, east=east, west=west):
            columns(t, [p - t for p in east] + [p + t for p in west])
            return carry
        lax.fori_loop(1, top + 1, wave, 0)
        if top == STEPS:
            for p in [p - STEPS for p in east] + [p + STEPS for p in west]:
                done(p)

    def store_back(n):
        return pltpu.make_async_copy(
            final.at[n],
            out.at[place(n), pl.ds(pl.multiple_of(half * (1 - s), EDGE), half)],
            store_sem.at[nlon + n],
        )

    for n in range(nlon):
        returns[n].wait_recv()
        store_back(nlon - 1 - n).start()

    for copy in small_near + swaps + direct + relays + returns:
        copy.wait_send()

    @pl.when(has_in)
    def _():
        for copy in small_in + edges_in:
            copy.wait_send()

    @pl.when(has_out)
    def _():
        for copy in small_out + edges_out:
            copy.wait_send()

    for n in range(nlon):
        store(n).wait()
        store_back(n).wait()


def body(field, kappa, classes, inverses):
    nlon, nlat, lev = field.shape
    span = 2 * (nlon + STEPS)
    half = nlat // 2
    total = half + 2 * PAD
    kinds = inverses.shape[0]
    vmem = pl.BlockSpec(memory_space=pltpu.VMEM)
    anywhere = pl.BlockSpec(memory_space=pl.ANY)
    dma = pltpu.SemaphoreType.DMA
    planes = 2 * nlon + 2 * STEPS
    edges = 2 + nlon + STEPS
    return pl.pallas_call(
        kernel,
        out_shape=jax.ShapeDtypeStruct(field.shape, F32),
        in_specs=[anywhere, vmem, vmem, vmem],
        out_specs=anywhere,
        scratch_shapes=[
            pltpu.VMEM((STEPS + 1, span, total, lev), F32),
            pltpu.VMEM((nlon, nlat, lev), F32),
            pltpu.VMEM((nlon, half, lev), F32),
            pltpu.VMEM((2, 4, nlon, nlat), F32),
            pltpu.VMEM((2, 4, nlon, nlat), jnp.int32),
            pltpu.VMEM((span, total, lev), F32),
            pltpu.VMEM((span, total, lev), F32),
            pltpu.VMEM((span, total, lev), F32),
            pltpu.VMEM((span, total - 2 * (PAD - EDGE), lev), BF16),
            pltpu.VMEM((span, total, lev), F32),
            pltpu.VMEM((6 * lev, kinds // 2 * lev), BF16),
            dma((nlon,)), dma((nlon,)), dma((2 * nlon,)),
            dma((7,)), dma((7,)), dma((7,)), dma((7,)),
            dma((edges,)), dma((edges,)), dma((planes,)), dma((planes,)),
        ],
        compiler_params=pltpu.CompilerParams(
            collective_id=0, has_side_effects=True, vmem_limit_bytes=60 * 1024 * 1024
        ),
    )(field, kappa, classes, inverses)


def solution(mesh):
    return jax.shard_map(
        body,
        mesh=mesh,
        in_specs=(P("lon", "lat", None), P("lon", "lat"), P("lon", "lat"), P()),
        out_specs=P("lon", "lat", None),
        check_vma=False,
    )
```
